32 devices in a mesh: peer: 8 (over y, x, core), zero: 4 (over z).
Axes of the slice: x: 2, y: 2, z: 4, core: 2. Of those that a mesh axis runs over, the one named last changes fastest.
Arguments:
- tokens: bfloat16 [8, 2048, 1024], P('peer', 'zero'), may hold values from -6 to 6
- out_grad: bfloat16 [8, 2048, 1024], P('peer', 'zero'), may hold values from -6 to 6
- step: int32 [1], replicated, may hold values from 0 to 3999
- up_param: float32 [8, 1024, 2048], P('peer', 'zero'), may hold values from -0.2 to 0.2
- down_param: float32 [8, 2048, 1024], P('peer', 'zero'), may hold values from -0.2 to 0.2
- up_first: float32 [8, 1024, 2048], P('peer', 'zero'), may hold values from -27.1529 to 27.1529
- down_first: float32 [8, 2048, 1024], P('peer', 'zero'), may hold values from -27.1529 to 27.1529
- up_second: float32 [8, 1024, 2048], P('peer', 'zero'), may hold values from 0.8192 to 819.2
- down_second: float32 [8, 2048, 1024], P('peer', 'zero'), may hold values from 0.8192 to 819.2
Outputs:
- new_up: float32 [8, 1024, 2048], P('peer', 'zero')
- new_down: float32 [8, 2048, 1024], P('peer', 'zero')
- new_up_first: float32 [8, 1024, 2048], P('peer', 'zero')
- new_down_first: float32 [8, 2048, 1024], P('peer', 'zero')
- new_up_second: float32 [8, 1024, 2048], P('peer', 'zero')
- new_down_second: float32 [8, 2048, 1024], P('peer', 'zero')
The draws below stay inside these ranges and needn't reach their ends.
All inputs are finite; a program needn't handle non-finite values.
Results may differ from the reference program's by a relative error of at most 0.0065.
Values may be sent and summed in bfloat16 or wider, within the bound.
A program may use at most 128 MiB of HBM per device.

```python
import math
import jax
import jax.numpy as jnp
from jax import lax

D = 1024
FFW = 2048
GTOK = 2048
GROUPS = 8
N_PEER = 8


def block_levels(key, shape, cuts, low, high):
    level = 1.0
    for position, blocks in cuts:
        steps = jax.random.uniform(jax.random.fold_in(jax.random.fold_in(key, 6), position), (blocks,), jnp.float32, low / len(cuts), high / len(cuts))
        level = level * jnp.repeat(jnp.exp(steps), shape[position] // blocks).reshape((-1,) + (1,) * (len(shape) - 1 - position))
    return level


def scatter_about(own_key, shape, width, limit, pieces=(), held_as=jnp.bfloat16):
    values = width * jax.random.normal(own_key, shape, jnp.float32)
    if pieces:
        values = values * block_levels(own_key, shape, pieces, -0.22, 0.18)
    return jnp.clip(values, -limit, limit).astype(held_as)


def setup_inputs(seed: int = 0) -> dict:
    splits = jax.random.split(jax.random.key(seed), 10)
    tokens = scatter_about(splits[0], (GROUPS, GTOK, D), 1.0, 6.0, ((0, 8), (1, 4)))
    out_grad = scatter_about(splits[1], (GROUPS, GTOK, D), 1.0, 6.0, ((0, 8), (1, 4)))
    step = jax.random.randint(splits[2], (1,), 0, 4000).astype(jnp.int32)
    up_param = scatter_about(splits[3], (GROUPS, D, FFW), 0.03, 0.2, ((0, 8), (1, 4)), jnp.float32)
    down_param = scatter_about(splits[4], (GROUPS, FFW, D), 0.03, 0.2, ((0, 8), (1, 4)), jnp.float32)
    up_first = scatter_about(splits[5], (GROUPS, D, FFW), (0.1 * GTOK ** 0.5), 27.1529, ((0, 8), (1, 4)), jnp.float32)
    down_first = scatter_about(splits[6], (GROUPS, FFW, D), (0.1 * GTOK ** 0.5), 27.1529, ((0, 8), (1, 4)), jnp.float32)
    up_second = jnp.clip(jnp.exp(math.log(819.2) - 6.9077553 * jax.random.uniform(splits[7], (GROUPS, D, FFW), jnp.float32) ** block_levels(splits[7], (GROUPS, D, FFW), ((0, 8), (1, 4)), -0.2, 0.2)), 0.8192, 819.2)
    down_second = jnp.clip(jnp.exp(math.log(819.2) - 6.9077553 * jax.random.uniform(splits[8], (GROUPS, FFW, D), jnp.float32) ** block_levels(splits[8], (GROUPS, FFW, D), ((0, 8), (1, 4)), -0.2, 0.2)), 0.8192, 819.2)
    return {"tokens": tokens, "out_grad": out_grad, "step": step, "up_param": up_param, "down_param": down_param, "up_first": up_first, "down_first": down_first, "up_second": up_second, "down_second": down_second}


def gelu_tanh(values):
    return 0.5 * values * (1.0 + jnp.tanh(0.7978845608 * (values + 0.044715 * values * values * values)))

def group_grads(items):
    tokens, out_grad, up_param, down_param = items
    widened = tokens.astype(jnp.float32)
    center = lax.optimization_barrier(jnp.mean(widened, axis=1, keepdims=True))
    spread = lax.optimization_barrier(jnp.mean((widened - center) * (widened - center), axis=1, keepdims=True))
    normed = ((widened - center) * lax.rsqrt(spread + 1e-05)).astype(jnp.bfloat16)
    up_low = up_param.astype(jnp.bfloat16)
    down_low = down_param.astype(jnp.bfloat16)
    pre = jnp.dot(normed, up_low, preferred_element_type=jnp.float32)
    active, backward = jax.vjp(gelu_tanh, pre)
    act = active.astype(jnp.bfloat16)
    act_grad = jnp.dot(out_grad, down_low.T, preferred_element_type=jnp.float32)
    pre_grad = backward(act_grad)[0].astype(jnp.bfloat16)
    up_grad = jnp.dot(normed.T, pre_grad, preferred_element_type=jnp.float32)
    down_grad = jnp.dot(act.T, out_grad, preferred_element_type=jnp.float32)
    return (up_grad, down_grad)

def adam_update(param, first, second, grad, first_fix, second_fix):
    first_new = 0.9 * first + 0.1 * grad
    second_new = 0.999 * second + 0.001 * grad * grad
    local = param - 0.01 * (first_new / first_fix) / (jnp.sqrt(second_new / second_fix) + 1e-08)
    return (local, first_new, second_new)

def reference(tokens, out_grad, step, up_param, down_param, up_first, down_first, up_second, down_second):
    up_grad, down_grad = lax.map(group_grads, (tokens, out_grad, up_param, down_param))
    count = (step[0] + 1).astype(jnp.float32)
    first_fix = 1.0 - jnp.power(jnp.float32(0.9), count)
    second_fix = 1.0 - jnp.power(jnp.float32(0.999), count)
    up_local, up_first_new, up_second_new = adam_update(up_param, up_first, up_second, up_grad, first_fix, second_fix)
    down_local, down_first_new, down_second_new = adam_update(down_param, down_first, down_second, down_grad, first_fix, second_fix)
    levels = N_PEER.bit_length() - 1
    distance = jnp.left_shift(jnp.int32(1), (step[0] % levels).astype(jnp.int32))
    partner = ((jnp.arange(N_PEER, dtype=jnp.int32) + distance) % N_PEER).astype(jnp.int32)
    new_up = 0.5 * (up_local + jnp.take(up_local, partner, axis=0))
    new_down = 0.5 * (down_local + jnp.take(down_local, partner, axis=0))
    return (new_up, new_down, up_first_new, down_first_new, up_second_new, down_second_new)
```

```python
from functools import partial

import jax
import jax.numpy as jnp
from jax import lax
from jax.experimental import pallas as pl
from jax.experimental.pallas import tpu as pltpu
from jax.sharding import PartitionSpec as P

MIB = 2**20


def passed_along(array, axis, by):
    size = lax.axis_size(axis)
    return lax.ppermute(array, axis, [(i, (i + by) % size) for i in range(size)])


def adam_update(param, first, second, grad, first_fix, second_fix):
    first_new = 0.9 * first + 0.1 * grad
    second_new = 0.999 * second + 0.001 * grad * grad
    local = param - 0.01 * (first_new / first_fix) / (jnp.sqrt(second_new / second_fix) + 1e-08)
    return (local, first_new, second_new)


def over_rows(left, right):
    return lax.dot_general(
        left, right, (((0,), (0,)), ((), ())), preferred_element_type=jnp.float32
    )


def grads_kernel(
    n,
    tile,
    own_tok,
    own_out,
    up_low,
    down_low,
    up_grad,
    down_grad,
    toks,
    outs,
    up_cols,
    up_sum,
    up_send,
    send_sem,
    recv_sem,
    w_send,
    w_recv,
    g_send,
    g_recv,
    local_sem,
):
    me = lax.axis_index("zero")
    rows, units = up_low.shape[0], down_low.shape[0]
    tokens = own_tok.shape[0]

    def peer(index):
        return {"zero": index}

    def remote(src, dst, send, recv, index):
        return pltpu.make_async_remote_copy(
            src_ref=src,
            dst_ref=dst,
            send_sem=send,
            recv_sem=recv,
            device_id=peer(index),
            device_id_type=pl.DeviceIdType.MESH,
        )

    def of(owner, size):
        return pl.ds(pl.multiple_of(owner * size, size), size)

    barrier = pltpu.get_barrier_semaphore()
    for hop in range(1, n):
        pl.semaphore_signal(
            barrier,
            inc=1,
            device_id=peer(lax.rem(me + hop, n)),
            device_id_type=pl.DeviceIdType.MESH,
        )
    pl.semaphore_wait(barrier, n - 1)

    def weights(hop):
        to = lax.rem(me + hop, n)
        return remote(
            up_low.at[:, of(to, units)],
            up_cols.at[of(me, rows)],
            w_send.at[hop],
            w_recv.at[hop],
            to,
        )

    for hop in range(1, n):
        weights(hop).start()

    arrays = ((own_tok, toks), (own_out, outs))

    def onward(side, which, owner):
        own, held = arrays[which]
        to = jnp.minimum(me + 1, n - 1) if side == 0 else jnp.maximum(me - 1, 0)
        return remote(
            held.at[owner],
            held.at[owner],
            send_sem.at[side, which, owner],
            recv_sem.at[which, owner],
            to,
        )

    def first(side, which):
        own, held = arrays[which]
        to = jnp.minimum(me + 1, n - 1) if side == 0 else jnp.maximum(me - 1, 0)
        return remote(
            own,
            held.at[me],
            send_sem.at[side, which, me],
            recv_sem.at[which, me],
            to,
        )

    has_right, has_left = me < n - 1, me > 0
    for which in range(2):

        @pl.when(has_right)
        def _():
            first(0, which).start()

        @pl.when(has_left)
        def _():
            first(1, which).start()

    keep = []
    for which, (own, held) in enumerate(arrays):
        keep.append(pltpu.make_async_copy(own, held.at[me], local_sem.at[which]))
    keep.append(
        pltpu.make_async_copy(
            up_low.at[:, of(me, units)], up_cols.at[of(me, rows)], local_sem.at[2]
        )
    )
    for copy in keep:
        copy.start()
    up_sum[...] = jnp.zeros_like(up_sum)
    down_grad[...] = jnp.zeros_like(down_grad)
    for copy in keep:
        copy.wait()
    for hop in range(1, n):
        weights(hop).wait()

    def compute(owner):
        @pl.loop(0, tokens // tile)
        def _(step):
            at = pl.ds(pl.multiple_of(step * tile, tile), tile)
            tok, out = toks[owner, at, :], outs[owner, at, :]
            pre = jnp.dot(tok, up_cols[...], preferred_element_type=jnp.float32)
            act_grad = lax.dot_general(
                out, down_low[...], (((1,), (1,)), ((), ())), preferred_element_type=jnp.float32
            )
            square = pre * pre
            bend = jnp.tanh(0.7978845608 * pre * (1.0 + 0.044715 * square))
            half = 0.5 * (1.0 + bend)
            act = (pre * half).astype(jnp.bfloat16)
            slope = half + 0.5 * pre * (1.0 - bend * bend) * (
                0.7978845608 * (1.0 + 3.0 * 0.044715 * square)
            )
            pre_grad = (act_grad * slope).astype(jnp.bfloat16)
            up_sum[...] += over_rows(tok, pre_grad)
            down_grad[...] += over_rows(act, out)

    @pl.loop(0, n)
    def _(k):
        left, right = me - k, me + k
        for which in range(2):

            @pl.when((k > 0) & (left >= 0))
            def _():
                onward(0, which, jnp.maximum(left, 0)).wait_recv()

                @pl.when(has_right)
                def _():
                    onward(0, which, jnp.maximum(left, 0)).start()

            @pl.when((k > 0) & (right < n))
            def _():
                onward(1, which, jnp.minimum(right, n - 1)).wait_recv()

                @pl.when(has_left)
                def _():
                    onward(1, which, jnp.minimum(right, n - 1)).start()

        for side in range(2):
            owner = left if side == 0 else right
            wanted = (owner >= 0) if side == 0 else ((k > 0) & (owner < n))

            @pl.when(wanted)
            def _():
                compute(jnp.clip(owner, 0, n - 1))

    up_send[...] = up_sum[...].astype(jnp.bfloat16)

    def back(hop):
        to = lax.rem(me + hop, n)
        return remote(
            up_send.at[of(to, rows)],
            up_grad.at[:, of(me, units)],
            g_send.at[hop],
            g_recv.at[hop],
            to,
        )

    for hop in range(1, n):
        back(hop).start()
    mine = pltpu.make_async_copy(
        up_send.at[of(me, rows)], up_grad.at[:, of(me, units)], local_sem.at[3]
    )
    mine.start()

    for which in range(2):
        for owner in range(n):

            @pl.when(has_right & (owner <= me))
            def _():
                onward(0, which, owner).wait_send()

            @pl.when(has_left & (owner >= me))
            def _():
                onward(1, which, owner).wait_send()

    mine.wait()
    for hop in range(1, n):
        back(hop).wait()


def group_grads(normed, out_grad, up_low, down_low):
    n = lax.axis_size("zero")
    tokens, width = normed.shape
    rows, hidden = up_low.shape
    units = down_low.shape[0]
    bf16, f32 = jnp.bfloat16, jnp.float32
    tile = min(tokens, 256)
    vmem = pl.BlockSpec(memory_space=pltpu.VMEM)
    dma = pltpu.SemaphoreType.DMA
    return pl.pallas_call(
        partial(grads_kernel, n, tile),
        out_shape=(
            jax.ShapeDtypeStruct((rows, hidden), bf16),
            jax.ShapeDtypeStruct((units, width), f32),
        ),
        in_specs=[vmem] * 4,
        out_specs=(vmem, vmem),
        scratch_shapes=[
            pltpu.VMEM((n, tokens, width), bf16),
            pltpu.VMEM((n, tokens, width), bf16),
            pltpu.VMEM((width, units), bf16),
            pltpu.VMEM((width, units), f32),
            pltpu.VMEM((width, units), bf16),
            dma((2, 2, n)),
            dma((2, n)),
            dma((n,)),
            dma((n,)),
            dma((n,)),
            dma((n,)),
            dma((4,)),
        ],
        compiler_params=pltpu.CompilerParams(
            collective_id=0, has_side_effects=True, vmem_limit_bytes=48 * MIB
        ),
    )(normed, out_grad, up_low, down_low)


def from_partner(pair, by):
    return passed_along(pair, "peer", -by)


def body(
    tokens, out_grad, step, up_param, down_param, up_first, down_first, up_second, down_second
):
    widened = tokens[0].astype(jnp.float32)
    center = jnp.mean(widened, axis=1, keepdims=True)
    spread = jnp.mean((widened - center) * (widened - center), axis=1, keepdims=True)
    normed = ((widened - center) * lax.rsqrt(spread + 1e-05)).astype(jnp.bfloat16)
    up_grad, down_grad = group_grads(
        normed,
        out_grad[0],
        up_param[0].astype(jnp.bfloat16),
        down_param[0].astype(jnp.bfloat16),
    )
    up_grad = up_grad.astype(jnp.float32)
    count = (step[0] + 1).astype(jnp.float32)
    first_fix = 1.0 - jnp.power(jnp.float32(0.9), count)
    second_fix = 1.0 - jnp.power(jnp.float32(0.999), count)
    up_local, up_first_new, up_second_new = adam_update(
        up_param[0], up_first[0], up_second[0], up_grad, first_fix, second_fix
    )
    down_local, down_first_new, down_second_new = adam_update(
        down_param[0], down_first[0], down_second[0], down_grad, first_fix, second_fix
    )
    levels = lax.axis_size("peer").bit_length() - 1
    branches = [partial(from_partner, by=2**level) for level in range(levels)]
    low = (up_local.astype(jnp.bfloat16), down_local.astype(jnp.bfloat16))
    up_other, down_other = lax.switch(step[0] % levels, branches, low)
    new_up = 0.5 * (up_local + up_other.astype(jnp.float32))
    new_down = 0.5 * (down_local + down_other.astype(jnp.float32))
    return (
        new_up[None],
        new_down[None],
        up_first_new[None],
        down_first_new[None],
        up_second_new[None],
        down_second_new[None],
    )


def solution(mesh):
    spec = P("peer", "zero", None)
    return jax.shard_map(
        body,
        mesh=mesh,
        in_specs=(spec, spec, P()) + (spec,) * 6,
        out_specs=(spec,) * 6,
        check_vma=False,
    )
```

```python
from functools import partial

import jax
import jax.numpy as jnp
from jax import lax
from jax.experimental import pallas as pl
from jax.experimental.pallas import tpu as pltpu
from jax.sharding import PartitionSpec as P

MIB = 2**20


def passed_along(array, axis, by):
    size = lax.axis_size(axis)
    return lax.ppermute(array, axis, [(i, (i + by) % size) for i in range(size)])


def adam_update(param, first, second, grad, first_fix, second_fix):
    first_new = 0.9 * first + 0.1 * grad
    second_new = 0.999 * second + 0.001 * grad * grad
    local = param - 0.01 * (first_new / first_fix) / (jnp.sqrt(second_new / second_fix) + 1e-08)
    return (local, first_new, second_new)


def over_rows(left, right):
    return lax.dot_general(
        left, right, (((0,), (0,)), ((), ())), preferred_element_type=jnp.float32
    )


def grads_kernel(
    n,
    tile,
    own_tok,
    own_out,
    up_low,
    down_low,
    up_low_grad,
    down_grad,
    toks,
    outs,
    up_cols,
    up_sum,
    send_sem,
    recv_sem,
    w_send,
    w_recv,
    local_sem,
):
    me = lax.axis_index("zero")
    rows, units = up_low.shape[0], down_low.shape[0]
    pieces = own_tok.shape[0] // tile

    def peer(index):
        return {"zero": index}

    def remote(src, dst, send, recv, index):
        return pltpu.make_async_remote_copy(
            src_ref=src,
            dst_ref=dst,
            send_sem=send,
            recv_sem=recv,
            device_id=peer(index),
            device_id_type=pl.DeviceIdType.MESH,
        )

    def of(owner, size):
        return pl.ds(pl.multiple_of(owner * size, size), size)

    barrier = pltpu.get_barrier_semaphore()
    for hop in range(1, n):
        pl.semaphore_signal(
            barrier,
            inc=1,
            device_id=peer(lax.rem(me + hop, n)),
            device_id_type=pl.DeviceIdType.MESH,
        )
    pl.semaphore_wait(barrier, n - 1)

    def weights(hop):
        to = lax.rem(me + hop, n)
        return remote(
            up_low.at[:, of(to, units)],
            up_cols.at[of(me, rows)],
            w_send.at[hop],
            w_recv.at[hop],
            to,
        )

    for hop in range(1, n):
        weights(hop).start()

    arrays = ((own_tok, toks), (own_out, outs))

    def part(piece):
        return pl.ds(piece * tile, tile)

    def onward(side, which, owner, piece, fresh=False):
        own, held = arrays[which]
        to = jnp.minimum(me + 1, n - 1) if side == 0 else jnp.maximum(me - 1, 0)
        return remote(
            own.at[part(piece)] if fresh else held.at[owner, part(piece)],
            held.at[owner, part(piece)],
            send_sem.at[side, which, owner, piece],
            recv_sem.at[which, owner, piece],
            to,
        )

    has_right, has_left = me < n - 1, me > 0
    for piece in range(pieces):
        for which in range(2):

            @pl.when(has_right)
            def _():
                onward(0, which, me, piece, True).start()

            @pl.when(has_left)
            def _():
                onward(1, which, me, piece, True).start()

    keep = []
    for which, (own, held) in enumerate(arrays):
        keep.append(pltpu.make_async_copy(own, held.at[me], local_sem.at[which]))
    keep.append(
        pltpu.make_async_copy(
            up_low.at[:, of(me, units)], up_cols.at[of(me, rows)], local_sem.at[2]
        )
    )
    for copy in keep:
        copy.start()
    up_sum[...] = jnp.zeros_like(up_sum)
    down_grad[...] = jnp.zeros_like(down_grad)
    for copy in keep:
        copy.wait()
    for hop in range(1, n):
        weights(hop).wait()

    def compute(owner, piece):
        tok, out = toks[owner, part(piece), :], outs[owner, part(piece), :]
        pre = jnp.dot(tok, up_cols[...], preferred_element_type=jnp.float32)
        act_grad = lax.dot_general(
            out, down_low[...], (((1,), (1,)), ((), ())), preferred_element_type=jnp.float32
        )
        square = pre * pre
        bend = jnp.tanh(0.7978845608 * pre * (1.0 + 0.044715 * square))
        half = 0.5 * (1.0 + bend)
        act = (pre * half).astype(jnp.bfloat16)
        slope = half + 0.5 * pre * (1.0 - bend * bend) * (
            0.7978845608 * (1.0 + 3.0 * 0.044715 * square)
        )
        pre_grad = (act_grad * slope).astype(jnp.bfloat16)
        up_sum[...] += over_rows(tok, pre_grad)
        down_grad[...] += over_rows(act, out)

    @pl.loop(0, n)
    def _(k):
        left, right = me - k, me + k
        lower, upper = jnp.maximum(left, 0), jnp.minimum(right, n - 1)
        for piece in range(pieces):
            for which in range(2):

                @pl.when((k > 0) & (left >= 0))
                def _():
                    onward(0, which, lower, piece).wait_recv()

                    @pl.when(has_right)
                    def _():
                        onward(0, which, lower, piece).start()

                @pl.when((k > 0) & (right < n))
                def _():
                    onward(1, which, upper, piece).wait_recv()

                    @pl.when(has_left)
                    def _():
                        onward(1, which, upper, piece).start()

            @pl.when(left >= 0)
            def _():
                compute(lower, piece)

            @pl.when((k > 0) & (right < n))
            def _():
                compute(upper, piece)

    up_low_grad[...] = up_sum[...].astype(jnp.bfloat16)

    for which in range(2):
        for owner in range(n):
            for piece in range(pieces):

                @pl.when(has_right & (owner <= me))
                def _():
                    onward(0, which, owner, piece).wait_send()

                @pl.when(has_left & (owner >= me))
                def _():
                    onward(1, which, owner, piece).wait_send()


def group_grads(normed, out_grad, up_low, down_low):
    n = lax.axis_size("zero")
    tokens, width = normed.shape
    units = down_low.shape[0]
    bf16, f32 = jnp.bfloat16, jnp.float32
    tile = min(tokens, 256)
    pieces = tokens // tile
    vmem = pl.BlockSpec(memory_space=pltpu.VMEM)
    dma = pltpu.SemaphoreType.DMA
    return pl.pallas_call(
        partial(grads_kernel, n, tile),
        out_shape=(
            jax.ShapeDtypeStruct((width, units), bf16),
            jax.ShapeDtypeStruct((units, width), f32),
        ),
        in_specs=[vmem] * 4,
        out_specs=(vmem, vmem),
        scratch_shapes=[
            pltpu.VMEM((n, tokens, width), bf16),
            pltpu.VMEM((n, tokens, width), bf16),
            pltpu.VMEM((width, units), bf16),
            pltpu.VMEM((width, units), f32),
            dma((2, 2, n, pieces)),
            dma((2, n, pieces)),
            dma((n,)),
            dma((n,)),
            dma((3,)),
        ],
        compiler_params=pltpu.CompilerParams(
            collective_id=0, has_side_effects=True, vmem_limit_bytes=48 * MIB
        ),
    )(normed, out_grad, up_low, down_low)


def rows_kernel(n, columns, whole, send_sem, recv_sem, local_sem):
    me = lax.axis_index("zero")
    rows, units = whole.shape[0], columns.shape[1]

    def of(owner, size):
        return pl.ds(pl.multiple_of(owner * size, size), size)

    barrier = pltpu.get_barrier_semaphore()
    for hop in range(1, n):
        pl.semaphore_signal(
            barrier,
            inc=1,
            device_id={"zero": lax.rem(me + hop, n)},
            device_id_type=pl.DeviceIdType.MESH,
        )
    pl.semaphore_wait(barrier, n - 1)
    copies = []
    for hop in range(1, n):
        to = lax.rem(me + hop, n)
        copies.append(
            pltpu.make_async_remote_copy(
                src_ref=columns.at[of(to, rows)],
                dst_ref=whole.at[:, of(me, units)],
                send_sem=send_sem.at[hop],
                recv_sem=recv_sem.at[hop],
                device_id={"zero": to},
                device_id_type=pl.DeviceIdType.MESH,
            )
        )
    copies.append(
        pltpu.make_async_copy(columns.at[of(me, rows)], whole.at[:, of(me, units)], local_sem.at[0])
    )
    for copy in copies:
        copy.start()
    for copy in copies:
        copy.wait()


def to_rows(columns):
    n = lax.axis_size("zero")
    width, units = columns.shape
    vmem = pl.BlockSpec(memory_space=pltpu.VMEM)
    dma = pltpu.SemaphoreType.DMA
    return pl.pallas_call(
        partial(rows_kernel, n),
        out_shape=jax.ShapeDtypeStruct((width // n, n * units), columns.dtype),
        in_specs=[vmem],
        out_specs=vmem,
        scratch_shapes=[dma((n,)), dma((n,)), dma((1,))],
        cost_estimate=pl.CostEstimate(
            flops=20 * 10**9, bytes_accessed=60 * MIB, transcendentals=0
        ),
        compiler_params=pltpu.CompilerParams(
            collective_id=1, has_side_effects=True, vmem_limit_bytes=16 * MIB
        ),
    )(columns)


def finish(operands, by):
    up_columns, up_state, down_local, fixes = operands
    down_other = passed_along(down_local.astype(jnp.bfloat16), "peer", -by)
    up_grad = to_rows(up_columns).astype(jnp.float32)
    up_local, up_first_new, up_second_new = adam_update(*up_state, up_grad, *fixes)
    up_other = passed_along(up_local.astype(jnp.bfloat16), "peer", -by)
    new_down = 0.5 * (down_local + down_other.astype(jnp.float32))
    new_up = 0.5 * (up_local + up_other.astype(jnp.float32))
    return new_up, new_down, up_first_new, up_second_new


def body(
    tokens, out_grad, step, up_param, down_param, up_first, down_first, up_second, down_second
):
    widened = tokens[0].astype(jnp.float32)
    center = jnp.mean(widened, axis=1, keepdims=True)
    spread = jnp.mean((widened - center) * (widened - center), axis=1, keepdims=True)
    normed = ((widened - center) * lax.rsqrt(spread + 1e-05)).astype(jnp.bfloat16)
    up_columns, down_grad = group_grads(
        normed,
        out_grad[0],
        up_param[0].astype(jnp.bfloat16),
        down_param[0].astype(jnp.bfloat16),
    )
    count = (step[0] + 1).astype(jnp.float32)
    first_fix = 1.0 - jnp.power(jnp.float32(0.9), count)
    second_fix = 1.0 - jnp.power(jnp.float32(0.999), count)
    down_local, down_first_new, down_second_new = adam_update(
        down_param[0], down_first[0], down_second[0], down_grad, first_fix, second_fix
    )
    levels = lax.axis_size("peer").bit_length() - 1
    branches = [partial(finish, by=2**level) for level in range(levels)]
    up_state = (up_param[0], up_first[0], up_second[0])
    operands = (up_columns, up_state, down_local, (first_fix, second_fix))
    new_up, new_down, up_first_new, up_second_new = lax.switch(
        step[0] % levels, branches, operands
    )
    return (
        new_up[None],
        new_down[None],
        up_first_new[None],
        down_first_new[None],
        up_second_new[None],
        down_second_new[None],
    )


def solution(mesh):
    spec = P("peer", "zero", None)
    return jax.shard_map(
        body,
        mesh=mesh,
        in_specs=(spec, spec, P()) + (spec,) * 6,
        out_specs=(spec,) * 6,
        check_vma=False,
    )
```
